32 devices in a mesh: seq: 8 (over z, y), tp: 4 (over x, core).
Axes of the slice: x: 2, y: 2, z: 4, core: 2. Of those that a mesh axis runs over, the one named last changes fastest.
Arguments:
- encoded: bfloat16 [8192, 1280], P(('seq', 'tp')), may hold values from -6 to 6
- starts: int32 [32, 32], replicated, may hold values from 0 to 256, as said below
- w_up: bfloat16 [1280, 4096], P(None, 'tp'), may hold values from -0.15625 to 0.15625
- norm_gain: float32 [4096], replicated, may hold values from 0.25 to 1.75
- w_query: bfloat16 [4096, 4096], P(None, 'tp'), may hold values from -8 to 8
- w_key: bfloat16 [4096, 4096], P(None, 'tp'), may hold values from -8 to 8
- w_value: bfloat16 [4096, 4096], P(None, 'tp'), may hold values from -0.09375 to 0.09375
- w_out: bfloat16 [4096, 4096], P('tp'), may hold values from -0.09375 to 0.09375
- cotangent: bfloat16 [1024, 4096], P('seq', 'tp'), may hold values from -6 to 6
Outputs:
- latent_out: bfloat16 [1024, 4096], P('seq', 'tp')
- latent_grad: float32 [1024, 4096], P('seq', 'tp')
The draws below stay inside these ranges and needn't reach their ends.
Inputs may be any that keep to these rules, and one draw needn't show every extreme that they name: `starts`: row i lists in increasing order the distinct offsets at which patches begin in byte shard i, followed by 256 in unused slots; every shard has at least one patch and at least 8, some shard exactly 32; shard 0 begins a patch at offset 0.
All inputs are finite; a program needn't handle non-finite values.
Results may differ from the reference program's by a relative error of at most 0.014.
Values may be sent and summed in bfloat16 or wider, within the bound.
A program may use at most 128 MiB of HBM per device.

```python
import jax
import jax.numpy as jnp
from jax import lax

E = 1280
D = 4096
HEADS = 32
HEAD_DIM = 128
B_DEV = 256
PATCH_CAP = 32
SHARDS = 32
PATCHES = 1024
BYTES = 8192


def shard_order(key):
    return jax.random.permutation(key, B_DEV)


def draw_starts(key, part):
    count_key, pick_key, full_key = jax.random.split(jax.random.fold_in(key, 3), 3)
    counts = jax.random.randint(count_key, (SHARDS,), max(PATCH_CAP // 4, 1), PATCH_CAP + 1)
    fullest = jax.random.randint(full_key, (), 0, SHARDS)
    counts = jnp.where(jnp.arange(SHARDS) == fullest, PATCH_CAP, counts)
    orders = jax.vmap(shard_order)(jax.random.split(pick_key, SHARDS))
    places = jnp.arange(B_DEV, dtype=jnp.int32)[None, :]
    chosen = jnp.where(orders < counts[:, None], places, B_DEV)
    ordered = jnp.sort(chosen, axis=1)[:, :PATCH_CAP]
    ordered = ordered.at[0, 0].set(0)
    return ordered.astype(jnp.int32)


def query_key_pair(key):
    first, second = jax.random.split(jax.random.fold_in(key, 17))
    query = jnp.clip(jax.random.normal(first, (D, D), jnp.float32), -5.0, 5.0) * D ** (-0.5)
    other = jnp.clip(jax.random.normal(second, (D, D), jnp.float32), -5.0, 5.0) * D ** (-0.5)
    keys = other
    return (query, keys)


def draw_w_query(key, part):
    return query_key_pair(key)[0].astype(jnp.bfloat16)


def draw_w_key(key, part):
    return query_key_pair(key)[1].astype(jnp.bfloat16)


def shard_levels(key, dims, cuts, least, high):
    def one(dim, parts):
        draws = jax.random.uniform(jax.random.fold_in(jax.random.fold_in(key, 6), dim), (parts,), jnp.float32, least / len(cuts), high / len(cuts))
        return jnp.repeat(jnp.exp(draws), dims[dim] // parts).reshape((-1,) + (1,) * (len(dims) - dim - 1))

    loudness = one(*cuts[0])
    for cut in cuts[1:]:
        loudness = loudness * one(*cut)
    return loudness


def bell_draw(rng, shape, spread, limit, cuts=(), kind=jnp.bfloat16):
    loudness = shard_levels(rng, shape, cuts, -0.22, 0.18) if cuts else 1.0
    drawn = jax.random.normal(rng, shape, jnp.float32) * spread * loudness
    return jnp.minimum(jnp.maximum(drawn, -limit), limit).astype(kind)


def setup_inputs(seed: int = 0) -> dict:
    key_list = jax.random.split(jax.random.key(seed), 10)
    encoded = bell_draw(key_list[0], (BYTES, E), 1.0, 6.0, ((0, 32),))
    starts = draw_starts(jax.random.fold_in(key_list[9], 71), 0)
    w_up = bell_draw(key_list[2], (E, D), E ** -0.5, 0.15625, ((1, 4),))
    norm_gain = jnp.clip(1.0 + 0.15 * jax.random.normal(key_list[3], (D,), jnp.float32), 0.25, 1.75)
    w_query = draw_w_query(jax.random.fold_in(key_list[9], 71), 0)
    w_key = draw_w_key(jax.random.fold_in(key_list[9], 71), 0)
    w_value = bell_draw(key_list[6], (D, D), D ** -0.5, 0.09375, ((1, 4),))
    w_out = bell_draw(key_list[7], (D, D), D ** -0.5, 0.09375, ((0, 4),))
    cotangent = bell_draw(key_list[8], (PATCHES, D), 1.0, 6.0, ((0, 8), (1, 4)))
    return {"encoded": encoded, "starts": starts, "w_up": w_up, "norm_gain": norm_gain, "w_query": w_query, "w_key": w_key, "w_value": w_value, "w_out": w_out, "cotangent": cotangent}


EPS = 1e-05
NEG = -1e+30
CONTRACT_LAST = (((1,), (1,)), ((), ()))

def pooled_patches(encoded, starts):
    shards = starts.shape[0]
    byte_blocks = encoded.reshape(shards, B_DEV, E).astype(jnp.float32)
    places = jnp.arange(B_DEV, dtype=jnp.int32)
    following = jnp.concatenate([starts[:, 1:], jnp.full((shards, 1), B_DEV, jnp.int32)], 1)
    member = ((places[None, None, :] >= starts[:, :, None]) & (places[None, None, :] < following[:, :, None])).astype(jnp.float32)
    sums = jnp.einsum('spb,sbe->spe', member, byte_blocks)
    sizes = lax.optimization_barrier(jnp.sum(member, 2))
    leading = (places[None, :] < starts[:, :1]).astype(jnp.float32)
    lead_sums = jnp.einsum('sb,sbe->se', leading, byte_blocks)
    lead_sizes = lax.optimization_barrier(jnp.sum(leading, 1))
    next_sums = jnp.concatenate([lead_sums[1:], jnp.zeros((1, E), jnp.float32)], 0)
    next_sizes = jnp.concatenate([lead_sizes[1:], jnp.zeros((1,), jnp.float32)], 0)
    counts = lax.optimization_barrier(jnp.sum((starts < B_DEV).astype(jnp.int32), 1))
    last_slot = (jnp.arange(PATCH_CAP, dtype=jnp.int32)[None, :] == (counts - 1)[:, None]).astype(jnp.float32)
    sums = sums + last_slot[:, :, None] * next_sums[:, None, :]
    sizes = sizes + last_slot * next_sizes[:, None]
    patches = sums / jnp.maximum(sizes, 1.0)[:, :, None]
    return patches.reshape(PATCHES, E).astype(jnp.bfloat16)

def split_heads(matrix):
    return matrix.reshape(PATCHES, HEADS, HEAD_DIM).transpose(1, 0, 2)

def join_heads(stacked):
    return stacked.transpose(1, 0, 2).reshape(PATCHES, D)

def reference(encoded, starts, w_up, norm_gain, w_query, w_key, w_value, w_out, cotangent):
    patches = pooled_patches(encoded, starts)
    valid = (starts < B_DEV).reshape(PATCHES)
    latent_in = jnp.dot(patches, w_up, preferred_element_type=jnp.float32).astype(jnp.bfloat16)
    wide = latent_in.astype(jnp.float32)
    rinv = lax.rsqrt(lax.optimization_barrier(jnp.sum(wide * wide, 1)) / D + EPS)
    scaled = (wide * norm_gain[None, :]).astype(jnp.bfloat16)
    query = (rinv[:, None] * jnp.dot(scaled, w_query, preferred_element_type=jnp.float32)).astype(jnp.bfloat16)
    keys = (rinv[:, None] * jnp.dot(scaled, w_key, preferred_element_type=jnp.float32)).astype(jnp.bfloat16)
    values = (rinv[:, None] * jnp.dot(scaled, w_value, preferred_element_type=jnp.float32)).astype(jnp.bfloat16)
    index = jnp.arange(PATCHES, dtype=jnp.int32)
    allowed = valid[None, :] & (index[None, :] <= index[:, None])
    scale = HEAD_DIM ** (-0.5)

    def head_forward(operands):
        head_query, head_key, head_value = operands
        scores = jnp.dot(head_query, head_key.T, preferred_element_type=jnp.float32) * scale
        peak = lax.optimization_barrier(jnp.max(jnp.where(allowed, scores, NEG), 1))
        expo = jnp.where(allowed, jnp.exp(scores - peak[:, None]), 0.0)
        total = lax.optimization_barrier(jnp.sum(expo, 1))
        mixed = jnp.dot(expo.astype(jnp.bfloat16), head_value, preferred_element_type=jnp.float32)
        return ((mixed / total[:, None]).astype(jnp.bfloat16), peak, total)
    heads_query = split_heads(query)
    heads_key = split_heads(keys)
    heads_value = split_heads(values)
    heads_attn, peaks, totals = lax.map(head_forward, (heads_query, heads_key, heads_value))
    attn = join_heads(heads_attn)
    result = wide + jnp.dot(attn, w_out, preferred_element_type=jnp.float32)
    latent_out = jnp.where(valid[:, None], result, 0.0).astype(jnp.bfloat16)
    grad_out = jnp.where(valid[:, None], cotangent, jnp.zeros_like(cotangent))
    d_attn = lax.dot_general(grad_out, w_out, CONTRACT_LAST, preferred_element_type=jnp.float32).astype(jnp.bfloat16)

    def head_backward(operands):
        head_query, head_key, head_value, head_out, head_grad, peak, total = operands
        scores = jnp.dot(head_query, head_key.T, preferred_element_type=jnp.float32) * scale
        probs = jnp.where(allowed, jnp.exp(scores - peak[:, None]), 0.0) / total[:, None]
        delta = lax.optimization_barrier(jnp.sum(head_grad.astype(jnp.float32) * head_out.astype(jnp.float32), 1))
        d_probs = jnp.dot(head_grad, head_value.T, preferred_element_type=jnp.float32)
        d_scores = (probs * (d_probs - delta[:, None])).astype(jnp.bfloat16)
        grad_query = (jnp.dot(d_scores, head_key, preferred_element_type=jnp.float32) * scale).astype(jnp.bfloat16)
        grad_key = (jnp.dot(d_scores.T, head_query, preferred_element_type=jnp.float32) * scale).astype(jnp.bfloat16)
        grad_value = jnp.dot(probs.astype(jnp.bfloat16).T, head_grad, preferred_element_type=jnp.float32).astype(jnp.bfloat16)
        return (grad_query, grad_key, grad_value)
    grads_query, grads_key, grads_value = lax.map(head_backward, (heads_query, heads_key, heads_value, heads_attn, split_heads(d_attn), peaks, totals))
    dnormed = lax.dot_general(join_heads(grads_query), w_query, CONTRACT_LAST, preferred_element_type=jnp.float32) + lax.dot_general(join_heads(grads_key), w_key, CONTRACT_LAST, preferred_element_type=jnp.float32) + lax.dot_general(join_heads(grads_value), w_value, CONTRACT_LAST, preferred_element_type=jnp.float32)
    dots = lax.optimization_barrier(jnp.sum(norm_gain[None, :] * dnormed * wide, 1))
    latent_grad = grad_out.astype(jnp.float32) + rinv[:, None] * norm_gain[None, :] * dnormed - wide * (rinv ** 3)[:, None] * dots[:, None] / D
    return (latent_out, latent_grad)
```

```python
import functools

import jax
import jax.numpy as jnp
from jax import lax
from jax.experimental import pallas as pl
from jax.experimental.pallas import tpu as pltpu
from jax.sharding import PartitionSpec as P

HEAD_DIM = 128


EPS = 1e-05
NEG = -1e30
CONTRACT_LAST = (((1,), (1,)), ((), ()))


def shifted(block, axis, distance):
    devices = range(lax.axis_size(axis))
    route = [(i - distance, i) for i in devices if i - distance in devices]
    return lax.ppermute(block, axis, route)


def per_device(encoded, starts, w_up, norm_gain, w_query, w_key, w_value, w_out, cotangent):
    byte_rows = encoded.shape[0]
    patch_cap = starts.shape[1]
    model_width = norm_gain.shape[0]
    shard = lax.axis_index(("seq", "tp"))
    own_starts = lax.dynamic_slice_in_dim(starts, shard, 1, 0)[0]
    places = jnp.arange(byte_rows, dtype=jnp.int32)
    following = jnp.concatenate([own_starts[1:], jnp.full((1,), byte_rows, jnp.int32)])
    inside = (places[None, :] >= own_starts[:, None]) & (places[None, :] < following[:, None])
    sums = jnp.dot(inside.astype(jnp.bfloat16), encoded, preferred_element_type=jnp.float32)
    sizes = jnp.sum(inside.astype(jnp.float32), 1)
    leading = places[None, :] < own_starts[:1, None]
    lead_sum = jnp.dot(leading.astype(jnp.bfloat16), encoded, preferred_element_type=jnp.float32)
    lead_size = jnp.sum(leading.astype(jnp.float32), 1)
    next_sum, next_size = shifted((lead_sum, lead_size), ("seq", "tp"), -1)
    count = jnp.sum((own_starts < byte_rows).astype(jnp.int32))
    last_slot = (jnp.arange(patch_cap, dtype=jnp.int32) == count - 1).astype(jnp.float32)
    sums = sums + last_slot[:, None] * next_sum
    sizes = sizes + last_slot * next_size
    patches = (sums / jnp.maximum(sizes, 1.0)[:, None]).astype(jnp.bfloat16)
    group = lax.all_gather(patches, "tp", axis=0, tiled=True)
    latent_in = jnp.dot(group, w_up, preferred_element_type=jnp.float32).astype(jnp.bfloat16)
    group_rows, columns = latent_in.shape
    head_count = columns // HEAD_DIM
    wide_piece = lax.all_gather(latent_in, "tp", axis=1, tiled=True).astype(jnp.float32)
    scaled = (wide_piece * norm_gain[None, :]).astype(jnp.bfloat16)
    acc_query = jnp.dot(scaled, w_query, preferred_element_type=jnp.float32)
    acc_key = jnp.dot(scaled, w_key, preferred_element_type=jnp.float32)
    acc_value = jnp.dot(scaled, w_value, preferred_element_type=jnp.float32)
    acc_query, acc_key, acc_value, square = (
        acc_query,
        acc_key,
        acc_value,
        jnp.sum(wide_piece * wide_piece, 1),
    )
    rinv = lax.rsqrt(square / model_width + EPS)
    query = (rinv[:, None] * acc_query).astype(jnp.bfloat16)
    key_rows = (rinv[:, None] * acc_key).astype(jnp.bfloat16)
    value_rows = (rinv[:, None] * acc_value).astype(jnp.bfloat16)
    keys_all, values_all = (
        lax.all_gather(key_rows, "seq", axis=0, tiled=True),
        lax.all_gather(value_rows, "seq", axis=0, tiled=True),
    )
    patches_total = keys_all.shape[0]
    valid_all = (starts < byte_rows).reshape(patches_total)
    row_base = lax.axis_index("seq") * group_rows
    query_index = row_base + jnp.arange(group_rows, dtype=jnp.int32)
    key_index = jnp.arange(patches_total, dtype=jnp.int32)
    query_valid = lax.dynamic_slice_in_dim(valid_all, row_base, group_rows, 0)
    allowed = valid_all[None, :] & (key_index[None, :] <= query_index[:, None])
    scale = HEAD_DIM ** (-0.5)
    query_heads = query.reshape(group_rows, head_count, HEAD_DIM)
    key_heads = keys_all.reshape(patches_total, head_count, HEAD_DIM)
    value_heads = values_all.reshape(patches_total, head_count, HEAD_DIM)
    scores = (
        jnp.einsum("rhd,khd->hrk", query_heads, key_heads, preferred_element_type=jnp.float32)
        * scale
    )
    peak = jnp.max(jnp.where(allowed[None], scores, NEG), 2)
    expo = jnp.where(allowed[None], jnp.exp(scores - peak[:, :, None]), 0.0)
    total = jnp.sum(expo, 2)
    mixed = jnp.einsum(
        "hrk,khd->rhd", expo.astype(jnp.bfloat16), value_heads, preferred_element_type=jnp.float32
    )
    attn = (mixed / total.T[:, :, None]).astype(jnp.bfloat16)
    partial_value = jnp.dot(
        attn.reshape(group_rows, columns), w_out, preferred_element_type=jnp.float32
    )
    head_sum = lax.psum_scatter(
        partial_value.astype(jnp.bfloat16), "tp", scatter_dimension=1, tiled=True
    ).astype(jnp.float32)
    wide_in = latent_in.astype(jnp.float32)
    latent_out = jnp.where(query_valid[:, None], wide_in + head_sum, 0.0).astype(jnp.bfloat16)
    grad_out = jnp.where(query_valid[:, None], cotangent, jnp.zeros_like(cotangent))
    d_attn = lax.dot_general(
        lax.all_gather(grad_out, "tp", axis=1, tiled=True),
        w_out,
        CONTRACT_LAST,
        preferred_element_type=jnp.float32,
    ).astype(jnp.bfloat16)
    grad_heads = d_attn.reshape(group_rows, head_count, HEAD_DIM)
    delta = jnp.sum(grad_heads.astype(jnp.float32) * attn.astype(jnp.float32), 2).T
    probs = expo / total[:, :, None]
    d_probs = jnp.einsum(
        "rhd,khd->hrk", grad_heads, value_heads, preferred_element_type=jnp.float32
    )
    d_scores = (probs * (d_probs - delta[:, :, None])).astype(jnp.bfloat16)
    grad_query = (
        (
            jnp.einsum("hrk,khd->rhd", d_scores, key_heads, preferred_element_type=jnp.float32)
            * scale
        )
        .astype(jnp.bfloat16)
        .reshape(group_rows, columns)
    )
    weights_low = probs.astype(jnp.bfloat16)
    count_rows = group_rows * lax.axis_size("seq")
    key_part = jnp.einsum("hrk,rhd->khd", d_scores, query_heads, preferred_element_type=jnp.float32)
    value_part = jnp.einsum(
        "hrk,rhd->khd", weights_low, grad_heads, preferred_element_type=jnp.float32
    )
    both = lax.psum_scatter(
        jnp.concatenate(
            [key_part.reshape(count_rows, columns), value_part.reshape(count_rows, columns)], 1
        ).astype(jnp.bfloat16),
        "seq",
        scatter_dimension=0,
        tiled=True,
    ).astype(jnp.float32)
    grad_key = (both[:, :columns] * scale).astype(jnp.bfloat16)
    grad_value = both[:, columns:].astype(jnp.bfloat16)
    dnormed = (
        lax.dot_general(grad_query, w_query, CONTRACT_LAST, preferred_element_type=jnp.float32)
        + lax.dot_general(grad_key, w_key, CONTRACT_LAST, preferred_element_type=jnp.float32)
        + lax.dot_general(grad_value, w_value, CONTRACT_LAST, preferred_element_type=jnp.float32)
    )
    normed_grad = lax.psum_scatter(
        dnormed.astype(jnp.bfloat16), "tp", scatter_dimension=1, tiled=True
    ).astype(jnp.float32)
    gain_own = lax.dynamic_slice_in_dim(norm_gain, lax.axis_index("tp") * columns, columns, 0)
    dots = lax.psum(jnp.sum(gain_own[None, :] * normed_grad * wide_in, 1), "tp")
    latent_grad = (
        grad_out.astype(jnp.float32)
        + rinv[:, None] * gain_own[None, :] * normed_grad
        - wide_in * (rinv**3)[:, None] * dots[:, None] / model_width
    )
    return (latent_out, latent_grad)


MESH = pl.DeviceIdType.MESH


def block(ref, dim, index, size):
    at = pl.ds(pl.multiple_of(index * size, size), size)
    return ref.at[at, :] if dim == 0 else ref.at[:, at]


def greet(axis, me, n):
    barrier = pltpu.get_barrier_semaphore()
    for offset in range(1, n):
        pl.semaphore_signal(
            barrier, inc=1, device_id={axis: lax.rem(me + offset, n)}, device_id_type=MESH
        )
    pl.semaphore_wait(barrier, n - 1)


def swap_kernel(axis, n, count, src_dim, dst_dim, *refs):
    sources, targets = refs[:count], refs[count : 2 * count]
    send_sem, recv_sem, own_sem = refs[2 * count :]
    me = lax.axis_index(axis)
    greet(axis, me, n)
    copies = []
    for i in range(count):
        src_size = sources[i].shape[src_dim] // n
        dst_size = targets[i].shape[dst_dim] // n
        landing = block(targets[i], dst_dim, me, dst_size)
        for offset in range(1, n):
            peer = lax.rem(me + offset, n)
            copy = pltpu.make_async_remote_copy(
                src_ref=block(sources[i], src_dim, peer, src_size),
                dst_ref=landing,
                send_sem=send_sem.at[i, offset],
                recv_sem=recv_sem.at[i, offset],
                device_id={axis: peer},
                device_id_type=MESH,
            )
            copy.start()
            copies.append(copy)
        own = pltpu.make_async_copy(
            block(sources[i], src_dim, me, src_size), landing, own_sem.at[i]
        )
        own.start()
        copies.append(own)
    for copy in copies:
        copy.wait()


def swap(arrays, axis, src_dim, dst_dim, collective_id):
    n, count = lax.axis_size(axis), len(arrays)
    shapes = []
    for array in arrays:
        shape = list(array.shape)
        shape[src_dim] //= n
        shape[dst_dim] *= n
        shapes.append(jax.ShapeDtypeStruct(tuple(shape), array.dtype))
    return pl.pallas_call(
        functools.partial(swap_kernel, axis, n, count, src_dim, dst_dim),
        out_shape=shapes,
        in_specs=[pl.BlockSpec(memory_space=pltpu.VMEM)] * count,
        out_specs=[pl.BlockSpec(memory_space=pltpu.VMEM)] * count,
        scratch_shapes=[
            pltpu.SemaphoreType.DMA((count, n)),
            pltpu.SemaphoreType.DMA((count, n)),
            pltpu.SemaphoreType.DMA((count,)),
        ],
        compiler_params=pltpu.CompilerParams(
            collective_id=collective_id, has_side_effects=True
        ),
    )(*arrays)


def collect_kernel(axis, n, count, dim, *refs):
    sources, targets = refs[:count], refs[count : 2 * count]
    send_sem, recv_sem, own_sem = refs[2 * count :]
    me = lax.axis_index(axis)
    partner = me + 1 - 2 * lax.rem(me, 2)
    half = n // 2
    greet(axis, me, n)

    def send(i, src, dst, slot, peer):
        copy = pltpu.make_async_remote_copy(
            src_ref=src,
            dst_ref=dst,
            send_sem=send_sem.at[i, slot],
            recv_sem=recv_sem.at[i, slot],
            device_id={axis: peer},
            device_id_type=MESH,
        )
        copy.start()
        return copy

    far, near = [], []
    for i in range(count):
        size = sources[i].shape[dim]
        for step in range(1, half):
            peer = lax.rem(me + 2 * step, n)
            landing = block(targets[i], dim, me, size)
            far.append((i, step, send(i, sources[i], landing, step, peer)))
    for i in range(count):
        landing = block(targets[i], dim, me, sources[i].shape[dim])
        near.append(send(i, sources[i], landing, 0, partner))
        own = pltpu.make_async_copy(sources[i], landing, own_sem.at[i])
        own.start()
        near.append(own)
    for i, step, copy in far:
        copy.wait_recv()
        origin = lax.rem(me + n - 2 * step, n)
        arrived = block(targets[i], dim, origin, sources[i].shape[dim])
        near.append(send(i, arrived, arrived, half + step, partner))
    for _, _, copy in far:
        copy.wait_send()
    for copy in near:
        copy.wait()


def collect(arrays, axis, dim, collective_id):
    n, count = lax.axis_size(axis), len(arrays)
    shapes = []
    for array in arrays:
        shape = list(array.shape)
        shape[dim] *= n
        shapes.append(jax.ShapeDtypeStruct(tuple(shape), array.dtype))
    return pl.pallas_call(
        functools.partial(collect_kernel, axis, n, count, dim),
        out_shape=shapes,
        in_specs=[pl.BlockSpec(memory_space=pltpu.VMEM)] * count,
        out_specs=[pl.BlockSpec(memory_space=pltpu.VMEM)] * count,
        scratch_shapes=[
            pltpu.SemaphoreType.DMA((count, n)),
            pltpu.SemaphoreType.DMA((count, n)),
            pltpu.SemaphoreType.DMA((count,)),
        ],
        compiler_params=pltpu.CompilerParams(
            collective_id=collective_id, has_side_effects=True
        ),
    )(*arrays)


def one_head(query, keys, values, d_attn, allowed):
    scale = HEAD_DIM ** (-0.5)
    scores = lax.dot_general(query, keys, CONTRACT_LAST, preferred_element_type=jnp.float32)
    scores = scores * scale
    peak = jnp.max(jnp.where(allowed, scores, NEG), 1)
    expo = jnp.where(allowed, jnp.exp(scores - peak[:, None]), 0.0)
    total = jnp.sum(expo, 1)
    mixed = jnp.dot(expo.astype(jnp.bfloat16), values, preferred_element_type=jnp.float32)
    attn = (mixed / total[:, None]).astype(jnp.bfloat16)
    delta = jnp.sum(d_attn.astype(jnp.float32) * attn.astype(jnp.float32), 1)
    probs = expo / total[:, None]
    d_probs = lax.dot_general(d_attn, values, CONTRACT_LAST, preferred_element_type=jnp.float32)
    d_scores = (probs * (d_probs - delta[:, None])).astype(jnp.bfloat16)
    rows = (((0,), (0,)), ((), ()))
    grad_query = jnp.dot(d_scores, keys, preferred_element_type=jnp.float32) * scale
    grad_key = lax.dot_general(d_scores, query, rows, preferred_element_type=jnp.float32) * scale
    grad_value = lax.dot_general(
        probs.astype(jnp.bfloat16), d_attn, rows, preferred_element_type=jnp.float32
    )
    low = jnp.bfloat16
    return attn, grad_query.astype(low), grad_key.astype(low), grad_value.astype(low)


def per_device_heads(encoded, starts, w_up, norm_gain, w_query, w_key, w_value, w_out, cotangent):
    byte_rows = encoded.shape[0]
    patch_cap = starts.shape[1]
    model_width = norm_gain.shape[0]
    shard = lax.axis_index(("seq", "tp"))
    own_starts = lax.dynamic_slice_in_dim(starts, shard, 1, 0)[0]
    places = jnp.arange(byte_rows, dtype=jnp.int32)
    following = jnp.concatenate([own_starts[1:], jnp.full((1,), byte_rows, jnp.int32)])
    inside = (places[None, :] >= own_starts[:, None]) & (places[None, :] < following[:, None])
    sums = jnp.dot(inside.astype(jnp.bfloat16), encoded, preferred_element_type=jnp.float32)
    sizes = jnp.sum(inside.astype(jnp.float32), 1)
    leading = places[None, :] < own_starts[:1, None]
    lead_sum = jnp.dot(leading.astype(jnp.bfloat16), encoded, preferred_element_type=jnp.float32)
    lead_size = jnp.sum(leading.astype(jnp.float32), 1)
    next_sum, next_size = shifted((lead_sum, lead_size), ("seq", "tp"), -1)
    count = jnp.sum((own_starts < byte_rows).astype(jnp.int32))
    last_slot = (jnp.arange(patch_cap, dtype=jnp.int32) == count - 1).astype(jnp.float32)
    sums = sums + last_slot[:, None] * next_sum
    sizes = sizes + last_slot * next_size
    patches = (sums / jnp.maximum(sizes, 1.0)[:, None]).astype(jnp.bfloat16)
    (group,) = collect([patches], "tp", 0, 0)
    latent_in = jnp.dot(group, w_up, preferred_element_type=jnp.float32).astype(jnp.bfloat16)
    group_rows, columns = latent_in.shape
    valid_all = (starts < byte_rows).reshape(starts.size)
    row_base = lax.axis_index("seq") * group_rows
    query_valid = lax.dynamic_slice_in_dim(valid_all, row_base, group_rows, 0)
    grad_out = jnp.where(query_valid[:, None], cotangent, jnp.zeros_like(cotangent))
    wide_low, wide_grad = collect([latent_in, grad_out], "tp", 1, 1)
    wide_piece = wide_low.astype(jnp.float32)
    scaled = (wide_piece * norm_gain[None, :]).astype(jnp.bfloat16)
    rinv = lax.rsqrt(jnp.sum(wide_piece * wide_piece, 1) / model_width + EPS)

    def project(weight):
        acc = jnp.dot(scaled, weight, preferred_element_type=jnp.float32)
        return (rinv[:, None] * acc).astype(jnp.bfloat16)

    d_attn_rows = lax.dot_general(
        wide_grad, w_out, CONTRACT_LAST, preferred_element_type=jnp.float32
    ).astype(jnp.bfloat16)
    query, keys, values, d_attn = swap(
        [project(w_query), project(w_key), project(w_value), d_attn_rows], "seq", 1, 0, 2
    )
    index = jnp.arange(starts.size, dtype=jnp.int32)
    allowed = valid_all[None, :] & (index[None, :] <= index[:, None])
    pieces = []
    for start in range(0, query.shape[1], HEAD_DIM):
        cut = slice(start, start + HEAD_DIM)
        pieces.append(one_head(query[:, cut], keys[:, cut], values[:, cut], d_attn[:, cut], allowed))
    joined = [p[0] if len(p) == 1 else jnp.concatenate(p, 1) for p in zip(*pieces)]
    attn, grad_query, grad_key, grad_value = swap(joined, "seq", 0, 1, 3)
    partial_value = jnp.dot(attn, w_out, preferred_element_type=jnp.float32).astype(jnp.bfloat16)
    dnormed = (
        lax.dot_general(grad_query, w_query, CONTRACT_LAST, preferred_element_type=jnp.float32)
        + lax.dot_general(grad_key, w_key, CONTRACT_LAST, preferred_element_type=jnp.float32)
        + lax.dot_general(grad_value, w_value, CONTRACT_LAST, preferred_element_type=jnp.float32)
    ).astype(jnp.bfloat16)
    value_parts, grad_parts = swap([partial_value, dnormed], "tp", 1, 0, 4)

    def add_up(parts):
        return jnp.sum(parts.reshape(-1, group_rows, columns).astype(jnp.float32), 0)

    wide_in = latent_in.astype(jnp.float32)
    latent_out = jnp.where(query_valid[:, None], wide_in + add_up(value_parts), 0.0)
    normed_grad = add_up(grad_parts)
    gain_own = lax.dynamic_slice_in_dim(norm_gain, lax.axis_index("tp") * columns, columns, 0)
    dots = lax.psum(jnp.sum(gain_own[None, :] * normed_grad * wide_in, 1), "tp")
    latent_grad = (
        grad_out.astype(jnp.float32)
        + rinv[:, None] * gain_own[None, :] * normed_grad
        - wide_in * (rinv**3)[:, None] * dots[:, None] / model_width
    )
    return (latent_out.astype(jnp.bfloat16), latent_grad)


def solution(mesh):
    in_specs = (
        P(("seq", "tp"), None),
        P(),
        P(None, "tp"),
        P(),
        P(None, "tp"),
        P(None, "tp"),
        P(None, "tp"),
        P("tp", None),
        P("seq", "tp"),
    )
    out_specs = (P("seq", "tp"), P("seq", "tp"))

    def choose(*arrays):
        heads = arrays[4].shape[1] // HEAD_DIM
        whole_heads = heads % lax.axis_size("seq") == 0 and lax.axis_size("tp") % 2 == 0
        return (per_device_heads if whole_heads else per_device)(*arrays)

    return jax.shard_map(
        choose, mesh=mesh, in_specs=in_specs, out_specs=out_specs, check_vma=False
    )
```

```python
import functools

import jax
import jax.numpy as jnp
from jax import lax
from jax.experimental import pallas as pl
from jax.experimental.pallas import tpu as pltpu
from jax.sharding import PartitionSpec as P

HEAD_DIM = 128


EPS = 1e-05
NEG = -1e30
CONTRACT_LAST = (((1,), (1,)), ((), ()))


def shifted(block, axis, distance):
    devices = range(lax.axis_size(axis))
    route = [(i - distance, i) for i in devices if i - distance in devices]
    return lax.ppermute(block, axis, route)


def per_device(encoded, starts, w_up, norm_gain, w_query, w_key, w_value, w_out, cotangent):
    byte_rows = encoded.shape[0]
    patch_cap = starts.shape[1]
    model_width = norm_gain.shape[0]
    shard = lax.axis_index(("seq", "tp"))
    own_starts = lax.dynamic_slice_in_dim(starts, shard, 1, 0)[0]
    places = jnp.arange(byte_rows, dtype=jnp.int32)
    following = jnp.concatenate([own_starts[1:], jnp.full((1,), byte_rows, jnp.int32)])
    inside = (places[None, :] >= own_starts[:, None]) & (places[None, :] < following[:, None])
    sums = jnp.dot(inside.astype(jnp.bfloat16), encoded, preferred_element_type=jnp.float32)
    sizes = jnp.sum(inside.astype(jnp.float32), 1)
    leading = places[None, :] < own_starts[:1, None]
    lead_sum = jnp.dot(leading.astype(jnp.bfloat16), encoded, preferred_element_type=jnp.float32)
    lead_size = jnp.sum(leading.astype(jnp.float32), 1)
    next_sum, next_size = shifted((lead_sum, lead_size), ("seq", "tp"), -1)
    count = jnp.sum((own_starts < byte_rows).astype(jnp.int32))
    last_slot = (jnp.arange(patch_cap, dtype=jnp.int32) == count - 1).astype(jnp.float32)
    sums = sums + last_slot[:, None] * next_sum
    sizes = sizes + last_slot * next_size
    patches = (sums / jnp.maximum(sizes, 1.0)[:, None]).astype(jnp.bfloat16)
    group = lax.all_gather(patches, "tp", axis=0, tiled=True)
    latent_in = jnp.dot(group, w_up, preferred_element_type=jnp.float32).astype(jnp.bfloat16)
    group_rows, columns = latent_in.shape
    head_count = columns // HEAD_DIM
    wide_piece = lax.all_gather(latent_in, "tp", axis=1, tiled=True).astype(jnp.float32)
    scaled = (wide_piece * norm_gain[None, :]).astype(jnp.bfloat16)
    acc_query = jnp.dot(scaled, w_query, preferred_element_type=jnp.float32)
    acc_key = jnp.dot(scaled, w_key, preferred_element_type=jnp.float32)
    acc_value = jnp.dot(scaled, w_value, preferred_element_type=jnp.float32)
    acc_query, acc_key, acc_value, square = (
        acc_query,
        acc_key,
        acc_value,
        jnp.sum(wide_piece * wide_piece, 1),
    )
    rinv = lax.rsqrt(square / model_width + EPS)
    query = (rinv[:, None] * acc_query).astype(jnp.bfloat16)
    key_rows = (rinv[:, None] * acc_key).astype(jnp.bfloat16)
    value_rows = (rinv[:, None] * acc_value).astype(jnp.bfloat16)
    keys_all, values_all = (
        lax.all_gather(key_rows, "seq", axis=0, tiled=True),
        lax.all_gather(value_rows, "seq", axis=0, tiled=True),
    )
    patches_total = keys_all.shape[0]
    valid_all = (starts < byte_rows).reshape(patches_total)
    row_base = lax.axis_index("seq") * group_rows
    query_index = row_base + jnp.arange(group_rows, dtype=jnp.int32)
    key_index = jnp.arange(patches_total, dtype=jnp.int32)
    query_valid = lax.dynamic_slice_in_dim(valid_all, row_base, group_rows, 0)
    allowed = valid_all[None, :] & (key_index[None, :] <= query_index[:, None])
    scale = HEAD_DIM ** (-0.5)
    query_heads = query.reshape(group_rows, head_count, HEAD_DIM)
    key_heads = keys_all.reshape(patches_total, head_count, HEAD_DIM)
    value_heads = values_all.reshape(patches_total, head_count, HEAD_DIM)
    scores = (
        jnp.einsum("rhd,khd->hrk", query_heads, key_heads, preferred_element_type=jnp.float32)
        * scale
    )
    peak = jnp.max(jnp.where(allowed[None], scores, NEG), 2)
    expo = jnp.where(allowed[None], jnp.exp(scores - peak[:, :, None]), 0.0)
    total = jnp.sum(expo, 2)
    mixed = jnp.einsum(
        "hrk,khd->rhd", expo.astype(jnp.bfloat16), value_heads, preferred_element_type=jnp.float32
    )
    attn = (mixed / total.T[:, :, None]).astype(jnp.bfloat16)
    partial_value = jnp.dot(
        attn.reshape(group_rows, columns), w_out, preferred_element_type=jnp.float32
    )
    head_sum = lax.psum_scatter(
        partial_value.astype(jnp.bfloat16), "tp", scatter_dimension=1, tiled=True
    ).astype(jnp.float32)
    wide_in = latent_in.astype(jnp.float32)
    latent_out = jnp.where(query_valid[:, None], wide_in + head_sum, 0.0).astype(jnp.bfloat16)
    grad_out = jnp.where(query_valid[:, None], cotangent, jnp.zeros_like(cotangent))
    d_attn = lax.dot_general(
        lax.all_gather(grad_out, "tp", axis=1, tiled=True),
        w_out,
        CONTRACT_LAST,
        preferred_element_type=jnp.float32,
    ).astype(jnp.bfloat16)
    grad_heads = d_attn.reshape(group_rows, head_count, HEAD_DIM)
    delta = jnp.sum(grad_heads.astype(jnp.float32) * attn.astype(jnp.float32), 2).T
    probs = expo / total[:, :, None]
    d_probs = jnp.einsum(
        "rhd,khd->hrk", grad_heads, value_heads, preferred_element_type=jnp.float32
    )
    d_scores = (probs * (d_probs - delta[:, :, None])).astype(jnp.bfloat16)
    grad_query = (
        (
            jnp.einsum("hrk,khd->rhd", d_scores, key_heads, preferred_element_type=jnp.float32)
            * scale
        )
        .astype(jnp.bfloat16)
        .reshape(group_rows, columns)
    )
    weights_low = probs.astype(jnp.bfloat16)
    count_rows = group_rows * lax.axis_size("seq")
    key_part = jnp.einsum("hrk,rhd->khd", d_scores, query_heads, preferred_element_type=jnp.float32)
    value_part = jnp.einsum(
        "hrk,rhd->khd", weights_low, grad_heads, preferred_element_type=jnp.float32
    )
    both = lax.psum_scatter(
        jnp.concatenate(
            [key_part.reshape(count_rows, columns), value_part.reshape(count_rows, columns)], 1
        ).astype(jnp.bfloat16),
        "seq",
        scatter_dimension=0,
        tiled=True,
    ).astype(jnp.float32)
    grad_key = (both[:, :columns] * scale).astype(jnp.bfloat16)
    grad_value = both[:, columns:].astype(jnp.bfloat16)
    dnormed = (
        lax.dot_general(grad_query, w_query, CONTRACT_LAST, preferred_element_type=jnp.float32)
        + lax.dot_general(grad_key, w_key, CONTRACT_LAST, preferred_element_type=jnp.float32)
        + lax.dot_general(grad_value, w_value, CONTRACT_LAST, preferred_element_type=jnp.float32)
    )
    normed_grad = lax.psum_scatter(
        dnormed.astype(jnp.bfloat16), "tp", scatter_dimension=1, tiled=True
    ).astype(jnp.float32)
    gain_own = lax.dynamic_slice_in_dim(norm_gain, lax.axis_index("tp") * columns, columns, 0)
    dots = lax.psum(jnp.sum(gain_own[None, :] * normed_grad * wide_in, 1), "tp")
    latent_grad = (
        grad_out.astype(jnp.float32)
        + rinv[:, None] * gain_own[None, :] * normed_grad
        - wide_in * (rinv**3)[:, None] * dots[:, None] / model_width
    )
    return (latent_out, latent_grad)


MESH = pl.DeviceIdType.MESH


def block(ref, dim, index, size):
    at = pl.ds(pl.multiple_of(index * size, size), size)
    return ref.at[at, :] if dim == 0 else ref.at[:, at]


def greet(axis, me, n):
    barrier = pltpu.get_barrier_semaphore()
    for offset in range(1, n):
        pl.semaphore_signal(
            barrier, inc=1, device_id={axis: lax.rem(me + offset, n)}, device_id_type=MESH
        )
    pl.semaphore_wait(barrier, n - 1)


def swap_kernel(axis, n, count, src_dim, dst_dim, *refs):
    sources, targets = refs[:count], refs[count : 2 * count]
    send_sem, recv_sem, own_sem = refs[2 * count :]
    me = lax.axis_index(axis)
    greet(axis, me, n)
    copies = []
    for i in range(count):
        src_size = sources[i].shape[src_dim] // n
        dst_size = targets[i].shape[dst_dim] // n
        landing = block(targets[i], dst_dim, me, dst_size)
        for offset in range(1, n):
            peer = lax.rem(me + offset, n)
            copy = pltpu.make_async_remote_copy(
                src_ref=block(sources[i], src_dim, peer, src_size),
                dst_ref=landing,
                send_sem=send_sem.at[i, offset],
                recv_sem=recv_sem.at[i, offset],
                device_id={axis: peer},
                device_id_type=MESH,
            )
            copy.start()
            copies.append(copy)
        own = pltpu.make_async_copy(
            block(sources[i], src_dim, me, src_size), landing, own_sem.at[i]
        )
        own.start()
        copies.append(own)
    for copy in copies:
        copy.wait()


def swap(arrays, axis, src_dim, dst_dim, collective_id):
    n, count = lax.axis_size(axis), len(arrays)
    shapes = []
    for array in arrays:
        shape = list(array.shape)
        shape[src_dim] //= n
        shape[dst_dim] *= n
        shapes.append(jax.ShapeDtypeStruct(tuple(shape), array.dtype))
    return pl.pallas_call(
        functools.partial(swap_kernel, axis, n, count, src_dim, dst_dim),
        out_shape=shapes,
        in_specs=[pl.BlockSpec(memory_space=pltpu.VMEM)] * count,
        out_specs=[pl.BlockSpec(memory_space=pltpu.VMEM)] * count,
        scratch_shapes=[
            pltpu.SemaphoreType.DMA((count, n)),
            pltpu.SemaphoreType.DMA((count, n)),
            pltpu.SemaphoreType.DMA((count,)),
        ],
        compiler_params=pltpu.CompilerParams(
            collective_id=collective_id, has_side_effects=True
        ),
    )(*arrays)


def collect_kernel(axis, n, count, dim, *refs):
    sources, targets = refs[:count], refs[count : 2 * count]
    send_sem, recv_sem, own_sem = refs[2 * count :]
    me = lax.axis_index(axis)
    partner = me + 1 - 2 * lax.rem(me, 2)
    half = n // 2
    greet(axis, me, n)

    def send(i, src, dst, slot, peer):
        copy = pltpu.make_async_remote_copy(
            src_ref=src,
            dst_ref=dst,
            send_sem=send_sem.at[i, slot],
            recv_sem=recv_sem.at[i, slot],
            device_id={axis: peer},
            device_id_type=MESH,
        )
        copy.start()
        return copy

    far, near = [], []
    for i in range(count):
        size = sources[i].shape[dim]
        for step in range(1, half):
            peer = lax.rem(me + 2 * step, n)
            landing = block(targets[i], dim, me, size)
            far.append((i, step, send(i, sources[i], landing, step, peer)))
    for i in range(count):
        landing = block(targets[i], dim, me, sources[i].shape[dim])
        near.append(send(i, sources[i], landing, 0, partner))
        own = pltpu.make_async_copy(sources[i], landing, own_sem.at[i])
        own.start()
        near.append(own)
    for i, step, copy in far:
        copy.wait_recv()
        origin = lax.rem(me + n - 2 * step, n)
        arrived = block(targets[i], dim, origin, sources[i].shape[dim])
        near.append(send(i, arrived, arrived, half + step, partner))
    for _, _, copy in far:
        copy.wait_send()
    for copy in near:
        copy.wait()


def collect(arrays, axis, dim, collective_id):
    n, count = lax.axis_size(axis), len(arrays)
    shapes = []
    for array in arrays:
        shape = list(array.shape)
        shape[dim] *= n
        shapes.append(jax.ShapeDtypeStruct(tuple(shape), array.dtype))
    return pl.pallas_call(
        functools.partial(collect_kernel, axis, n, count, dim),
        out_shape=shapes,
        in_specs=[pl.BlockSpec(memory_space=pltpu.VMEM)] * count,
        out_specs=[pl.BlockSpec(memory_space=pltpu.VMEM)] * count,
        scratch_shapes=[
            pltpu.SemaphoreType.DMA((count, n)),
            pltpu.SemaphoreType.DMA((count, n)),
            pltpu.SemaphoreType.DMA((count,)),
        ],
        compiler_params=pltpu.CompilerParams(
            collective_id=collective_id, has_side_effects=True
        ),
    )(*arrays)


def one_head(query, keys, values, d_attn, allowed):
    scale = HEAD_DIM ** (-0.5)
    scores = lax.dot_general(query, keys, CONTRACT_LAST, preferred_element_type=jnp.float32)
    scores = scores * scale
    peak = jnp.max(jnp.where(allowed, scores, NEG), 1)
    expo = jnp.where(allowed, jnp.exp(scores - peak[:, None]), 0.0)
    total = jnp.sum(expo, 1)
    mixed = jnp.dot(expo.astype(jnp.bfloat16), values, preferred_element_type=jnp.float32)
    attn = (mixed / total[:, None]).astype(jnp.bfloat16)
    delta = jnp.sum(d_attn.astype(jnp.float32) * attn.astype(jnp.float32), 1)
    probs = expo / total[:, None]
    d_probs = lax.dot_general(d_attn, values, CONTRACT_LAST, preferred_element_type=jnp.float32)
    d_scores = (probs * (d_probs - delta[:, None])).astype(jnp.bfloat16)
    rows = (((0,), (0,)), ((), ()))
    grad_query = jnp.dot(d_scores, keys, preferred_element_type=jnp.float32) * scale
    grad_key = lax.dot_general(d_scores, query, rows, preferred_element_type=jnp.float32) * scale
    grad_value = lax.dot_general(
        probs.astype(jnp.bfloat16), d_attn, rows, preferred_element_type=jnp.float32
    )
    low = jnp.bfloat16
    return attn, grad_query.astype(low), grad_key.astype(low), grad_value.astype(low)


def per_device_heads(encoded, starts, w_up, norm_gain, w_query, w_key, w_value, w_out, cotangent):
    byte_rows = encoded.shape[0]
    patch_cap = starts.shape[1]
    model_width = norm_gain.shape[0]
    shard = lax.axis_index(("seq", "tp"))
    own_starts = lax.dynamic_slice_in_dim(starts, shard, 1, 0)[0]
    places = jnp.arange(byte_rows, dtype=jnp.int32)
    following = jnp.concatenate([own_starts[1:], jnp.full((1,), byte_rows, jnp.int32)])
    inside = (places[None, :] >= own_starts[:, None]) & (places[None, :] < following[:, None])
    sums = jnp.dot(inside.astype(jnp.bfloat16), encoded, preferred_element_type=jnp.float32)
    sizes = jnp.sum(inside.astype(jnp.float32), 1)
    leading = places[None, :] < own_starts[:1, None]
    lead_sum = jnp.dot(leading.astype(jnp.bfloat16), encoded, preferred_element_type=jnp.float32)
    lead_size = jnp.sum(leading.astype(jnp.float32), 1)
    next_sum, next_size = shifted((lead_sum, lead_size), ("seq", "tp"), -1)
    count = jnp.sum((own_starts < byte_rows).astype(jnp.int32))
    last_slot = (jnp.arange(patch_cap, dtype=jnp.int32) == count - 1).astype(jnp.float32)
    sums = sums + last_slot[:, None] * next_sum
    sizes = sizes + last_slot * next_size
    patches = (sums / jnp.maximum(sizes, 1.0)[:, None]).astype(jnp.bfloat16)
    (group,) = collect([patches], "tp", 0, 0)
    latent_in = jnp.dot(group, w_up, preferred_element_type=jnp.float32).astype(jnp.bfloat16)
    group_rows, columns = latent_in.shape
    valid_all = (starts < byte_rows).reshape(starts.size)
    row_base = lax.axis_index("seq") * group_rows
    query_valid = lax.dynamic_slice_in_dim(valid_all, row_base, group_rows, 0)
    grad_out = jnp.where(query_valid[:, None], cotangent, jnp.zeros_like(cotangent))
    wide_low, wide_grad = collect([latent_in, grad_out], "tp", 1, 1)
    wide_piece = wide_low.astype(jnp.float32)
    scaled = (wide_piece * norm_gain[None, :]).astype(jnp.bfloat16)
    rinv = lax.rsqrt(jnp.sum(wide_piece * wide_piece, 1) / model_width + EPS)

    def project(weight):
        acc = jnp.dot(scaled, weight, preferred_element_type=jnp.float32)
        return (rinv[:, None] * acc).astype(jnp.bfloat16)

    d_attn_rows = lax.dot_general(
        wide_grad, w_out, CONTRACT_LAST, preferred_element_type=jnp.float32
    ).astype(jnp.bfloat16)
    query, keys, values, d_attn = swap(
        [project(w_query), project(w_key), project(w_value), d_attn_rows], "seq", 1, 0, 2
    )
    index = jnp.arange(starts.size, dtype=jnp.int32)
    allowed = valid_all[None, :] & (index[None, :] <= index[:, None])
    pieces = []
    for start in range(0, query.shape[1], HEAD_DIM):
        cut = slice(start, start + HEAD_DIM)
        pieces.append(one_head(query[:, cut], keys[:, cut], values[:, cut], d_attn[:, cut], allowed))
    joined = [p[0] if len(p) == 1 else jnp.concatenate(p, 1) for p in zip(*pieces)]
    attn, grad_query, grad_key, grad_value = swap(joined, "seq", 0, 1, 3)
    partial_value = jnp.dot(attn, w_out, preferred_element_type=jnp.float32).astype(jnp.bfloat16)
    dnormed = (
        lax.dot_general(grad_query, w_query, CONTRACT_LAST, preferred_element_type=jnp.float32)
        + lax.dot_general(grad_key, w_key, CONTRACT_LAST, preferred_element_type=jnp.float32)
        + lax.dot_general(grad_value, w_value, CONTRACT_LAST, preferred_element_type=jnp.float32)
    ).astype(jnp.bfloat16)
    dot_parts = jnp.sum(norm_gain[None, :] * dnormed.astype(jnp.float32) * wide_piece, 1)
    tp_size = lax.axis_size("tp")
    dot_tile = jnp.broadcast_to(jnp.tile(dot_parts, tp_size)[None, :], (8, tp_size * group_rows))
    value_parts, grad_parts, dot_rows = swap([partial_value, dnormed, dot_tile], "tp", 1, 0, 4)
    dots = jnp.sum(dot_rows.reshape(tp_size, 8, group_rows)[:, 0], 0)

    def add_up(parts):
        return jnp.sum(parts.reshape(-1, group_rows, columns).astype(jnp.float32), 0)

    wide_in = latent_in.astype(jnp.float32)
    latent_out = jnp.where(query_valid[:, None], wide_in + add_up(value_parts), 0.0)
    normed_grad = add_up(grad_parts)
    gain_own = lax.dynamic_slice_in_dim(norm_gain, lax.axis_index("tp") * columns, columns, 0)
    latent_grad = (
        grad_out.astype(jnp.float32)
        + rinv[:, None] * gain_own[None, :] * normed_grad
        - wide_in * (rinv**3)[:, None] * dots[:, None] / model_width
    )
    return (latent_out.astype(jnp.bfloat16), latent_grad)


def solution(mesh):
    in_specs = (
        P(("seq", "tp"), None),
        P(),
        P(None, "tp"),
        P(),
        P(None, "tp"),
        P(None, "tp"),
        P(None, "tp"),
        P("tp", None),
        P("seq", "tp"),
    )
    out_specs = (P("seq", "tp"), P("seq", "tp"))

    def choose(*arrays):
        heads = arrays[4].shape[1] // HEAD_DIM
        whole_heads = heads % lax.axis_size("seq") == 0 and lax.axis_size("tp") % 2 == 0
        return (per_device_heads if whole_heads else per_device)(*arrays)

    return jax.shard_map(
        choose, mesh=mesh, in_specs=in_specs, out_specs=out_specs, check_vma=False
    )
```
